32 devices in a mesh: seg: 4 (over y, x), tile: 8 (over z, core).
Axes of the slice: x: 2, y: 2, z: 4, core: 2. Of those that a mesh axis runs over, the one named last changes fastest.
Arguments:
- starting_warmth: float32 [256, 65536], P('tile', 'seg'), may hold values from 0 to 1
- diffusivity_field: float32 [256, 65536], P('tile', 'seg'), may hold values from 0.1 to 1
- emitter_mask: int32 [256, 65536], P('tile', 'seg'), may hold values 0 or 1
Outputs:
- final_warmth: float32 [256, 65536], P('tile', 'seg')
The draws below stay inside these ranges and needn't reach their ends.
Inputs may be any that keep to these rules, and one draw needn't show every extreme that they name: `emitter_mask`: nonzero marks a source vertex.
All inputs are finite; a program needn't handle non-finite values. No bound on the sum of `emitter_mask` on one device may be relied on, other than what follows from the above.
Results may differ from the reference program's by a relative error of at most 0.00002.
Values sent between devices are 32-bit elements; how exact they have to be, the bound alone decides.
A program may use at most 128 MiB of HBM per device.

```python
import math
import jax
import jax.numpy as jnp

STEPS = 8
BAND_BREADTH = 256
BAND_EXTENT = 65536


def with_ends(values, rng, smallest, high):
    dims = values.shape
    index_at = [jax.random.randint(jax.random.fold_in(rng, axis), (), 0, dims[axis]) for axis in range(len(dims))]
    values = values.at[tuple(index_at)].set(smallest)
    longest = dims.index(max(dims))
    index_at[longest] = (index_at[longest] + 1) % dims[longest]
    return values.at[tuple(index_at)].set(high)


def block_scale(stream_key, shape, cuts, smallest, high):
    def one(axis_at, blocks):
        draws = jax.random.uniform(jax.random.fold_in(jax.random.fold_in(stream_key, 6), axis_at), (blocks,), jnp.float32, smallest / len(cuts), high / len(cuts))
        return jnp.repeat(jnp.exp(draws), shape[axis_at] // blocks).reshape((-1,) + (1,) * (len(shape) - axis_at - 1))

    loudness = one(*cuts[0])
    for cut in cuts[1:]:
        loudness = loudness * one(*cut)
    return loudness


def setup_inputs(seed: int = 0) -> dict:
    streams_of = jax.random.split(jax.random.key(seed), 4)
    return {
        "starting_warmth": jnp.clip(1.0 * jax.random.uniform(streams_of[0], (BAND_BREADTH, BAND_EXTENT), jnp.float32) ** block_scale(streams_of[0], (BAND_BREADTH, BAND_EXTENT), ((0, 8), (1, 4)), -0.2, 0.2), 0.0, 1.0),
        "diffusivity_field": jnp.clip(jnp.exp(math.log(1.0) - 2.3025851 * jax.random.uniform(streams_of[1], (BAND_BREADTH, BAND_EXTENT), jnp.float32) ** block_scale(streams_of[1], (BAND_BREADTH, BAND_EXTENT), ((0, 8), (1, 4)), -0.2, 0.2)), 0.1, 1.0),
        "emitter_mask": with_ends((jax.random.randint(streams_of[2], (BAND_BREADTH, BAND_EXTENT), 0, 64) < 1).astype(jnp.int32), jax.random.fold_in(streams_of[2], 1), 0, 1),
    }


time_step = 0.24


def advance(bordered_grid, conduct, source, interior_region):
    height = bordered_grid.shape[0] - 2
    length = bordered_grid.shape[1] - 2
    middle_point = bordered_grid[1:-1, 1:-1]
    self_conductance = conduct[1:-1, 1:-1]
    flux_sum = jnp.zeros_like(middle_point)
    for row_off, col_off in ((0, 1), (2, 1), (1, 0), (1, 2)):
        adjacent_cell = bordered_grid[row_off:row_off + height, col_off:col_off + length]
        near_conduct = conduct[row_off:row_off + height, col_off:col_off + length]
        flux_sum = flux_sum + 0.5 * (self_conductance + near_conduct) * (adjacent_cell - middle_point)
    updated = middle_point + time_step * flux_sum
    updated = jnp.where(source, jnp.float32(1.0), updated)
    if interior_region is not None:
        updated = updated * interior_region
    return updated


def reference(starting_warmth, diffusivity_field, emitter_mask):
    is_source = emitter_mask != 0
    conduct = jnp.pad(diffusivity_field, 1)
    present_warmth = starting_warmth
    for substep in range(STEPS):
        present_warmth = advance(jnp.pad(present_warmth, 1), conduct, is_source, None)
    return present_warmth
```

```python
import functools

import jax
import jax.numpy as jnp
from jax import lax
from jax.experimental import pallas as pl
from jax.experimental.pallas import tpu as pltpu
from jax.sharding import PartitionSpec as P

STEPS = 8
ROUNDS = (1, 3, 4)
PLAN = (
    ("near", 0), ("far", 0), ("fill", 4), ("near", 1), ("fill", 5), ("far", 1),
    ("fill", 8), ("give", 0), ("near", 2), ("far", 2),
)
assert ROUNDS[0] == 1 and ROUNDS[1] > 1
START = tuple(sum(ROUNDS[:m]) for m in range(len(ROUNDS) + 1))
DEEP = max(ROUNDS)
STEP_SIZE = 0.24
LANES = 128
SUB = 8
MESH = pl.DeviceIdType.MESH

PAD = 16
TERMS = 4
VMEM_KERNEL = 50 * 1024 * 1024
VMEM_LAST = 1024 * 1024
TERM_ROWS = 5 * SUB
FIELDS = 3


def chunks():
    have, found = 0, []
    for d in ROUNDS:
        found.append((have, max(have, d)))
        have = max(have, d)
    return found


CHUNKS = chunks()


def kernel(
    sizes, u_hbm, k_hbm, s_hbm, out,
    u_nat, k_nat, s_nat,
    u_0, u_a, u_b, k_row, w_row, coef,
    marks_in, col_out, col_in, corner_in, packed_ref, row_out, row_in,
    load_sem, edge_sem, col_sems, corner_sems, first_sems, row_sems,
):
    rows, blocks, n_seg, n_tile = sizes
    groups = rows // SUB
    n = len(ROUNDS)
    soon = ROUNDS[1]
    seg, tile = lax.axis_index("seg"), lax.axis_index("tile")
    lane = lax.broadcasted_iota(jnp.int32, (SUB, LANES), 1)
    sublane = lax.broadcasted_iota(jnp.int32, (SUB, LANES), 0)
    first_lane, last_lane = lane == 0, lane == LANES - 1
    has_side = (seg > 0, seg < n_seg - 1)
    has_row = (tile > 0, tile < n_tile - 1)
    side_step = (-1, 1)
    own_at = PAD + SUB
    halo_at = (PAD, own_at + LANES)
    edge_at = (own_at, own_at + LANES - SUB)
    edge_lane = (first_lane, last_lane)
    edge_id = (0, LANES - 1)
    parts = LANES // SUB
    length = LANES + 2 * SUB + 2 * PAD
    zero, half = jnp.float32(0.0), jnp.float32(0.5 * STEP_SIZE)
    own = pl.ds(own_at, LANES)
    wide = pl.ds(PAD, LANES + 2 * SUB)
    per_group = FIELDS * SUB
    near = 1 - tile % 2
    far = tile % 2

    def both(a, b):
        return jnp.logical_and(a, b)

    def there_is(side):
        other = tile + 2 * side - 1
        return both(other >= 0, other < n_tile)

    def pick(side, a, b):
        return a + side * (b - a)

    def span_at(side, lo, hi):
        return pick(side, DEEP + lo, DEEP + rows - hi)

    def row_at(side, r):
        return pick(side, DEEP + r, DEEP + rows - 1 - r)

    barrier = pltpu.get_barrier_semaphore()
    count = jnp.int32(0)
    for ds in (-1, 0, 1):
        for dt in (-1, 0, 1):
            if ds == 0 and dt == 0:
                continue
            there = jnp.bool_(True)
            if ds:
                there = has_side[(ds + 1) // 2]
            if dt:
                there = both(there, has_row[(dt + 1) // 2])
            count = count + there.astype(jnp.int32)

            @pl.when(there)
            def _(ds=ds, dt=dt):
                pl.semaphore_signal(barrier, inc=1, device_id=(seg + ds, tile + dt), device_id_type=MESH)

    span = blocks * SUB
    sources = ((u_hbm, u_nat), (k_hbm, k_nat), (s_hbm, s_nat))

    def load(which, g):
        src, dst = sources[which]
        return pltpu.make_async_copy(src.at[g], dst.at[g], load_sem.at[which, g])

    def edge_load(which, side):
        at = pl.ds(0 if side == 0 else (blocks - 1) * SUB, SUB)
        dst = marks_in.at[side] if which == 2 else col_out.at[side, which]
        return pltpu.make_async_copy(sources[which][0].at[:, at], dst, edge_sem.at[which, side])

    for side in range(2):
        for which in range(3):
            edge_load(which, side).start()

    for which in range(2):
        for g in (0, groups - 1):
            load(which, g).start()

    zero_plane = jnp.zeros((SUB, LANES), jnp.float32)
    for side in range(2):
        top = 0 if side == 0 else DEEP + rows

        @pl.when(jnp.logical_not(has_row[side]))
        def _(top=top):
            def clear(j, c):
                at = pl.ds(j * SUB, SUB)
                for d in range(DEEP):
                    for ref in (u_0, u_a, u_b, k_row):
                        ref[top + d, at, :] = zero_plane
                    w_row[top + d, at, :] = zero_plane + half
                return c

            lax.fori_loop(0, length // SUB, clear, 0)

    def relay_heat(row, g, at):
        u_0[DEEP + row, own, :] = u_nat[g, at, :].T

    def relay_rest(row, g, at):
        k = k_nat[g, at, :]
        marked = jnp.where(s_nat[g, at, :] != 0, -k, k).T
        k_row[DEEP + row, own, :] = jnp.abs(marked)
        w_row[DEEP + row, own, :] = jnp.where(marked < 0.0, zero, half)

    def place(row):
        return row, row // SUB, pl.ds(row % SUB, LANES, stride=SUB)

    def relay_k(row, g, at):
        k_row[DEEP + row, own, :] = k_nat[g, at, :].T

    def relay_mark(row, g, at):
        w_row[DEEP + row, own, :] = jnp.where(s_nat[g, at, :] != 0, zero, half).T

    def pair(r):
        return place(r), place(rows - 1 - r)

    def relay_range(relay, lo):
        amount = rows - 2 * lo
        step = max(d for d in range(1, 16) if amount % d == 0)

        def body(i, c):
            for q in range(step):
                relay(*place(lo + i * step + q))
            return c

        lax.fori_loop(0, amount // step, body, 0)

    def first_copy(m, which, side, arriving):
        lo, hi = CHUNKS[m]
        if which == 0:
            ref, lo, hi = u_0, 0, ROUNDS[0]
        elif which == 1:
            ref = k_row
        else:
            ref, lo, hi = w_row, max(lo - 1, 0), hi - 1
        if hi <= lo:
            return None
        mine = span_at(side, lo, hi)
        theirs = pick(side, DEEP + rows + lo, DEEP - hi)
        halo = pick(side, DEEP - hi, DEEP + rows + lo)
        src = ref.at[pl.ds(halo if arriving else mine, hi - lo), own]
        dst = ref.at[pl.ds(halo if arriving else theirs, hi - lo), own]
        other = side if arriving else 1 - side
        return pltpu.make_async_remote_copy(
            src_ref=src, dst_ref=dst,
            send_sem=first_sems.at[0, m, which, side], recv_sem=first_sems.at[1, m, which, other],
            device_id=(seg, tile + pick(side, -1, 1)), device_id_type=MESH,
        )

    def first_fields(m):
        return [w for w in range(3) if (w or m == 0) and (w == 0 or CHUNKS[m][1] > CHUNKS[m][0])]

    def first_send(m, side):
        @pl.when(there_is(side))
        def _():
            for which in first_fields(m):
                copy = first_copy(m, which, side, False)
                if copy is not None:
                    copy.start()

    def col_copy(side):
        return pltpu.make_async_remote_copy(
            src_ref=col_out.at[side], dst_ref=col_in.at[1 - side],
            send_sem=col_sems.at[0, side], recv_sem=col_sems.at[1, 1 - side],
            device_id=(seg + side_step[side], tile), device_id_type=MESH,
        )

    def corner_copy(side, vert):
        g = 0 if vert == 0 else groups - 1
        return pltpu.make_async_remote_copy(
            src_ref=col_out.at[side, :, g], dst_ref=corner_in.at[1 - side, 1 - vert],
            send_sem=corner_sems.at[0, side, vert], recv_sem=corner_sems.at[1, 1 - side, 1 - vert],
            device_id=(seg + side_step[side], tile + side_step[vert]), device_id_type=MESH,
        )

    for g in (0, groups - 1):
        load(2, g).start()
    for which in range(3):
        for g in range(1, groups - 1):
            load(which, g).start()

    for side in range(2):
        for which in range(3):
            edge_load(which, side).wait()
        for g in range(groups):
            col_out[side, 2, g] = jnp.where(marks_in[side, g] != 0, zero, half)
    pl.semaphore_wait(barrier, count)
    for side in range(2):
        @pl.when(has_side[side])
        def _(side=side):
            col_copy(side).start()

        for vert in range(2):
            @pl.when(both(has_side[side], has_row[vert]))
            def _(side=side, vert=vert):
                corner_copy(side, vert).start()

    ends = (0, groups - 1)
    for which in range(2):
        for g in ends:
            load(which, g).wait()
    for where in pair(0):
        relay_heat(*where)
        relay_k(*where)
    for side in range(2):
        first_send(0, side)
    for g in ends:
        load(2, g).wait()
    for where in pair(0):
        relay_mark(*where)
    for r in range(1, soon):
        for where in pair(r):
            relay_rest(*where)
    for side in range(2):
        first_send(1, side)
    for r in range(1, soon + 1):
        for where in pair(r):
            relay_heat(*where)
    for where in pair(soon):
        relay_rest(*where)
    for which in range(3):
        for g in range(1, groups - 1):
            load(which, g).wait()
    relay_range(relay_heat, soon + 1)
    relay_range(relay_rest, soon + 1)

    def prepare(start, amount, halo=None, first=0, end=parts + 2, unroll=1, inner=False):
        def body(g, c):
            base = pl.multiple_of(g * SUB, SUB) + PAD
            at = pl.ds(base, SUB)
            if not inner:
                cell = base - own_at + sublane
                outside = both(both(seg == 0, first_lane), cell < 0)
                outside = jnp.logical_or(outside, both(both(seg == n_seg - 1, last_lane), cell >= LANES))
                inside = jnp.logical_not(outside)
            here = k_row[start, at, :]
            north = here + k_row[start - 1, at, :]
            for i in range(amount):
                row = start + i
                below = k_row[row + 1, at, :]
                weight = w_row[row, at, :]
                if not inner:
                    live = inside
                    if halo is not None:
                        live = both(live, halo(i))
                    weight = jnp.where(live, weight, zero)
                south = here + below
                cw = weight * (here + k_row[row, pl.ds(base - 1, SUB), :])
                ce = weight * (here + k_row[row, pl.ds(base + 1, SUB), :])
                for t, term in enumerate((ce, cw, weight * north, weight * south)):
                    coef[row, pl.ds(pl.multiple_of(g * TERM_ROWS, SUB) + t * SUB, SUB), :] = term
                here, north = below, south
            return c

        lax.fori_loop(first, end, body, 0, unroll=unroll)

    def field(level):
        return u_0 if level == 0 else (u_a if level % 2 == 1 else u_b)

    def advance(j, ranges, unroll=1, first=None, end=None):
        src, dst = field(j - 1), field(j)
        last = j == STEPS

        def body(g, c):
            base = pl.multiple_of(g * SUB, SUB) + PAD
            at = pl.ds(base, SUB)
            for start, amount in ranges:
                here = src[start, at, :]
                rise = here - src[start - 1, at, :]
                for i in range(amount):
                    row = start + i
                    below = src[row + 1, at, :]
                    ce, cw, cn, cs = (
                        coef[row, pl.ds(pl.multiple_of(g * TERM_ROWS, SUB) + t * SUB, SUB), :] for t in range(TERMS)
                    )
                    fall = below - here
                    new = here + (
                        (cs * fall - cn * rise)
                        + (ce * (src[row, pl.ds(base + 1, SUB), :] - here) + cw * (src[row, pl.ds(base - 1, SUB), :] - here))
                    )
                    if j == 1:
                        new = jnp.where(w_row[row, at, :] == 0.0, jnp.float32(1.0), new)
                    dst[row, at, :] = new
                    here, rise = below, fall
            return c

        first = (1 if last else 0) if first is None else first
        end = parts + (1 if last else 2) if end is None else end
        lax.fori_loop(first, end, body, 0, unroll=unroll)

    prepare(DEEP + 1, rows - 2, first=2, end=parts, inner=True)
    advance(1, [(DEEP + 1, rows - 2)], first=2, end=parts)

    row_refs = (u_0, k_row, w_row)

    absent = jnp.where((lane // SUB) % FIELDS == FIELDS - 1, half, zero)
    absent_col = jnp.where(lane >= (FIELDS - 1) * rows, half, zero)

    def packed_of(ref, side):
        a, b = ref.shape[1:3]
        tiles_of = [ref[side, p, q] for p in range(a) for q in range(b)]
        turned = jnp.concatenate(tiles_of + [zero_plane] * (parts - a * b)).T
        return turned[-SUB:] if side == 0 else turned[:SUB]

    def patch(ref, row, side, packed, at_lane):
        end = ref[row, edge_at[1 - side]:edge_at[1 - side] + SUB, :]
        end = pltpu.roll(end, (1, LANES - 1)[side], 1)
        got = pltpu.roll(packed, (edge_id[side] - at_lane) % LANES, 1)
        ref[row, halo_at[side]:halo_at[side] + SUB, :] = jnp.where(edge_lane[side], got, end)

    for side in range(2):
        @pl.when(has_side[side])
        def _(side=side):
            col_copy(1 - side).wait_recv()
    packed_col = [jnp.where(has_side[side], packed_of(col_in, side), absent_col) for side in range(2)]

    def patch_rows(which_rows):
        for side in range(2):
            for r in which_rows:
                for which, ref in enumerate(row_refs):
                    patch(ref, DEEP + r, side, packed_col[side], which * rows + r)

    def sides_of(start, amount):
        for first, end in ((0, 2), (parts, parts + 2)):
            prepare(start, amount, first=first, end=end, unroll=2 if amount < SUB else 1)
            advance(1, [(start, amount)], first=first, end=end, unroll=2 if amount < SUB else 1)

    at_ends = list(range(soon + 1))
    patch_rows(at_ends + [rows - 1 - r for r in at_ends])
    for side in range(2):
        sides_of(span_at(side, 1, soon), soon - 1)

    def row_copy(m, side, early, arriving=False):
        cut = min(ROUNDS[m - 1], ROUNDS[m])
        part = pl.ds(cut, ROUNDS[m] - cut) if early else pl.ds(0, cut)
        other = side if arriving else 1 - side
        return pltpu.make_async_remote_copy(
            src_ref=row_out.at[m - 1, side, part], dst_ref=row_in.at[m - 1, other, part],
            send_sem=row_sems.at[0, m - 1, side, int(early)], recv_sem=row_sems.at[1, m - 1, other, int(early)],
            device_id=(seg, tile + pick(side, -1, 1)), device_id_type=MESH,
        )

    def is_early(m):
        return ROUNDS[m] > ROUNDS[m - 1]

    def row_send(m, side, early):
        cut = min(ROUNDS[m - 1], ROUNDS[m])
        src = field(START[m])

        @pl.when(there_is(side))
        def _():
            for r in range(cut, ROUNDS[m]) if early else range(cut):
                row_out[m - 1, side, r, :, :] = src[row_at(side, r), wide, :]
            row_copy(m, side, early).start()

    def row_take(m, side):
        dst = field(START[m])

        @pl.when(there_is(side))
        def _():
            row_copy(m, side, False, True).wait_recv()
            if is_early(m):
                row_copy(m, side, True, True).wait_recv()
            for r in range(ROUNDS[m]):
                dst[row_at(side, -1 - r), wide, :] = row_in[m - 1, side, r, :, :]

    def halo_rows(m, side):
        lo, hi = CHUNKS[m]

        @pl.when(there_is(side))
        def _():
            for which in first_fields(m):
                copy = first_copy(m, which, side, True)
                if copy is not None:
                    copy.wait_recv()
            for side_of in range(2):
                packed = packed_ref[side_of]
                for which, ref in enumerate(row_refs):
                    if which not in first_fields(m):
                        continue
                    a, b = (lo, hi) if which == 1 else (0, ROUNDS[0]) if which == 0 else (max(lo - 1, 0), hi - 1)
                    for r in range(a, b):
                        at_lane = pick(side, SUB - 1 - r, per_group + r) + which * SUB
                        patch(ref, row_at(side, -1 - r), side_of, packed, at_lane)

        low, high = -(hi - 1), (1 if m == 0 else -(lo - 1))
        start, amount = span_at(side, low, high), high - low

        def halo(i):
            is_halo = jnp.logical_or(start + i < DEEP, start + i >= DEEP + rows)
            return jnp.logical_or(jnp.logical_not(is_halo), there_is(side))

        prepare(start, amount, halo, unroll=6)

    done = {1: 1}
    early_sent = {1}

    def note(j, low):
        done[j] = low
        for m in range(1, n):
            if m not in early_sent and is_early(m) and START[m] == j and low <= ROUNDS[m - 1]:
                early_sent.add(m)
                for side in range(2):
                    row_send(m, side, True)

    def step_all(j, low):
        if j not in done:
            advance(j, [(DEEP + low, rows - 2 * low)])
        elif done[j] > low:
            amount = done[j] - low
            advance(j, [(span_at(side, low, done[j]), amount) for side in range(2)], unroll=2)
        note(j, low)

    def give(row):
        out[row // SUB, pl.ds(row % SUB, LANES, stride=SUB), :] = field(STEPS)[DEEP + row, own, :].T

    for side in range(2):
        row_send(1, side, True)

    for side in range(2):
        for vert in range(2):
            @pl.when(both(has_side[side], has_row[vert]))
            def _(side=side, vert=vert):
                corner_copy(1 - side, 1 - vert).wait_recv()
        packed_ref[side] = jnp.where(has_side[side], packed_of(corner_in, side), absent)

    reached = 0
    for what, arg in PLAN:
        if what == "fill":
            for j in range(START[reached] + 1, arg + 1):
                step_all(j, j - START[reached])
        elif what == "give":
            edge = ROUNDS[n - 1]

            def give_more(i, c, edge=edge):
                give(edge + i)
                return c

            lax.fori_loop(0, rows - 2 * edge, give_more, 0, unroll=8 if (rows - 2 * edge) % 8 == 0 else 2)
        else:
            m, side = arg, near if what == "near" else far
            if m:
                row_take(m, side)
            if CHUNKS[m][1] > CHUNKS[m][0]:
                halo_rows(m, side)
            for j in range(START[m] + 1, START[m + 1] + 1):
                low, high = j - START[m + 1], done[j]
                advance(j, [(span_at(side, low, high), high - low)], unroll=6 if j < STEPS else 4)
            if m + 1 < n:
                row_send(m + 1, side, False)
                if m + 2 < n:
                    first_send(m + 2, side)
            else:
                for i in range(ROUNDS[m]):
                    give(span_at(side, 0, ROUNDS[m]) - DEEP + i)
            if what == "far":
                reached = m + 1
                if m == 0:
                    patch_rows(range(soon + 1, rows - soon - 1))
                    sides_of(DEEP + soon, rows - 2 * soon)
                for j in range(START[m] + 1, START[m + 1] + 1):
                    note(j, j - START[m + 1])

    for side in range(2):
        @pl.when(has_side[side])
        def _(side=side):
            col_copy(side).wait_send()

        for vert in range(2):
            @pl.when(both(has_side[side], has_row[vert]))
            def _(side=side, vert=vert):
                corner_copy(side, vert).wait_send()

        @pl.when(has_row[side])
        def _(side=side):
            for m in range(n):
                for which in first_fields(m):
                    copy = first_copy(m, which, side, False)
                    if copy is not None:
                        copy.wait_send()
            for m in range(1, n):
                row_copy(m, side, False).wait_send()
                if is_early(m):
                    row_copy(m, side, True).wait_send()


def write_out(src, dst, sems):
    copies = [pltpu.make_async_copy(src.at[g], dst.at[g], sems.at[g]) for g in range(src.shape[0])]
    for copy in copies:
        copy.start()
    for copy in copies:
        copy.wait()


def shards(n_seg, n_tile, warmth, conductivity, sources):
    rows, columns = warmth.shape
    blocks = columns // LANES
    groups = rows // SUB

    def planes(a):
        return a.reshape(groups, SUB, blocks, LANES).transpose(0, 2, 1, 3).reshape(groups, -1, LANES)

    flat = (groups, SUB * blocks, LANES)
    f32 = jnp.float32
    length = LANES + 2 * SUB + 2 * PAD
    plane = (rows + 2 * DEEP, length, LANES)
    assert blocks == LANES
    vmem = pltpu.VMEM
    sem = pltpu.SemaphoreType.DMA
    n = len(ROUNDS)
    later = max(n - 1, 1)
    halo = (later, 2, DEEP, LANES + 2 * SUB, LANES)
    out = pl.pallas_call(
        functools.partial(kernel, (rows, blocks, n_seg, n_tile)),
        out_shape=jax.ShapeDtypeStruct(flat, f32),
        in_specs=[pl.BlockSpec(memory_space=pltpu.HBM)] * 3,
        out_specs=pl.BlockSpec(memory_space=pltpu.VMEM),
        scratch_shapes=[
            vmem(flat, f32), vmem(flat, f32), vmem(flat, sources.dtype),
        ] + [vmem(plane, f32)] * 5 + [
            vmem((rows + 2 * DEEP, (LANES // SUB + 2) * TERM_ROWS, LANES), f32),
            vmem((2, groups, SUB, LANES), sources.dtype), vmem((2, FIELDS, groups, SUB, LANES), f32),
            vmem((2, FIELDS, groups, SUB, LANES), f32), vmem((2, 2, FIELDS, SUB, LANES), f32), vmem((2, SUB, LANES), f32),
            vmem(halo, f32), vmem(halo, f32),
            sem((3, groups)), sem((3, 2)), sem((2, 2)), sem((2, 2, 2)), sem((2, n, 3, 2)), sem((2, later, 2, 2)),
        ],
        compiler_params=pltpu.CompilerParams(
            collective_id=0, has_side_effects=True, vmem_limit_bytes=VMEM_KERNEL
        ),
    )(planes(warmth), planes(conductivity), planes(sources))
    out = pl.pallas_call(
        write_out,
        out_shape=jax.ShapeDtypeStruct(flat, f32),
        in_specs=[pl.BlockSpec(memory_space=pl.ANY)],
        out_specs=pl.BlockSpec(memory_space=pltpu.HBM),
        scratch_shapes=[sem((groups,))],
        compiler_params=pltpu.CompilerParams(vmem_limit_bytes=VMEM_LAST),
    )(out)
    return out.reshape(groups, blocks, SUB, LANES).transpose(0, 2, 1, 3).reshape(rows, columns)


def solution(mesh):
    spec = P("tile", "seg")
    return jax.shard_map(
        functools.partial(shards, mesh.shape["seg"], mesh.shape["tile"]),
        mesh=mesh,
        in_specs=(spec, spec, spec),
        out_specs=spec,
        check_vma=False,
    )
```

```python
import functools

import jax
import jax.numpy as jnp
from jax import lax
from jax.experimental import pallas as pl
from jax.experimental.pallas import tpu as pltpu
from jax.sharding import PartitionSpec as P

STEPS = 8
ROUNDS = (1, 3, 4)
PLAN = (
    ("far", 0), ("near", 0), ("fill", 4), ("far", 1), ("near", 1), ("fill", 8), ("give", 0), ("near", 2), ("far", 2),
)
assert ROUNDS[0] == 1 and ROUNDS[1] > 1
START = tuple(sum(ROUNDS[:m]) for m in range(len(ROUNDS) + 1))
DEEP = max(ROUNDS)
STEP_SIZE = 0.24
LANES = 128
SUB = 8
MESH = pl.DeviceIdType.MESH

PAD = 16
TERMS = 4
VMEM_KERNEL = 50 * 1024 * 1024
VMEM_LAST = 1024 * 1024
TERM_ROWS = 5 * SUB
FIELDS = 3


def chunks():
    have, found = 0, []
    for d in ROUNDS:
        found.append((have, max(have, d)))
        have = max(have, d)
    return found


CHUNKS = chunks()


def kernel(
    sizes, u_hbm, k_hbm, s_hbm, out,
    u_nat, k_nat, s_nat,
    u_0, u_a, u_b, k_row, w_row, coef,
    marks_in, col_out, col_in, corner_in, packed_ref, row_out, row_in,
    load_sem, edge_sem, col_sems, corner_sems, first_sems, row_sems,
):
    rows, blocks, n_seg, n_tile = sizes
    groups = rows // SUB
    n = len(ROUNDS)
    soon = ROUNDS[1]
    seg, tile = lax.axis_index("seg"), lax.axis_index("tile")
    lane = lax.broadcasted_iota(jnp.int32, (SUB, LANES), 1)
    sublane = lax.broadcasted_iota(jnp.int32, (SUB, LANES), 0)
    first_lane, last_lane = lane == 0, lane == LANES - 1
    has_side = (seg > 0, seg < n_seg - 1)
    has_row = (tile > 0, tile < n_tile - 1)
    side_step = (-1, 1)
    own_at = PAD + SUB
    halo_at = (PAD, own_at + LANES)
    edge_at = (own_at, own_at + LANES - SUB)
    edge_lane = (first_lane, last_lane)
    edge_id = (0, LANES - 1)
    parts = LANES // SUB
    length = LANES + 2 * SUB + 2 * PAD
    zero, half = jnp.float32(0.0), jnp.float32(0.5 * STEP_SIZE)
    own = pl.ds(own_at, LANES)
    wide = pl.ds(PAD, LANES + 2 * SUB)
    per_group = FIELDS * SUB
    near = 1 - tile % 2
    far = tile % 2

    def both(a, b):
        return jnp.logical_and(a, b)

    def there_is(side):
        other = tile + 2 * side - 1
        return both(other >= 0, other < n_tile)

    def pick(side, a, b):
        return a + side * (b - a)

    def span_at(side, lo, hi):
        return pick(side, DEEP + lo, DEEP + rows - hi)

    def row_at(side, r):
        return pick(side, DEEP + r, DEEP + rows - 1 - r)

    barrier = pltpu.get_barrier_semaphore()
    count = jnp.int32(0)
    for ds in (-1, 0, 1):
        for dt in (-1, 0, 1):
            if ds == 0 and dt == 0:
                continue
            there = jnp.bool_(True)
            if ds:
                there = has_side[(ds + 1) // 2]
            if dt:
                there = both(there, has_row[(dt + 1) // 2])
            count = count + there.astype(jnp.int32)

            @pl.when(there)
            def _(ds=ds, dt=dt):
                pl.semaphore_signal(barrier, inc=1, device_id=(seg + ds, tile + dt), device_id_type=MESH)

    span = blocks * SUB
    sources = ((u_hbm, u_nat), (k_hbm, k_nat), (s_hbm, s_nat))

    ends = (0, groups - 1)

    def load(which, g, amount=1):
        src, dst = sources[which]
        part = pl.ds(g, amount)
        sem = load_sem.at[2 + which if amount > 1 else which // 2]
        return pltpu.make_async_copy(src.at[part], dst.at[part], sem)

    def loaded(ref, sem):
        pltpu.make_async_copy(ref, ref, sem).wait()

    def edge_load(which, side):
        at = pl.ds(0 if side == 0 else (blocks - 1) * SUB, SUB)
        dst = marks_in.at[side] if which == 2 else col_out.at[side, which]
        return pltpu.make_async_copy(sources[which][0].at[:, at], dst, edge_sem.at[which // 2])

    for side in range(2):
        for which in range(3):
            edge_load(which, side).start()

    for which in range(2):
        for g in ends:
            load(which, g).start()

    zero_plane = jnp.zeros((SUB, LANES), jnp.float32)
    for side in range(2):
        top = 0 if side == 0 else DEEP + rows

        @pl.when(jnp.logical_not(has_row[side]))
        def _(top=top):
            def clear(j, c):
                at = pl.ds(j * SUB, SUB)
                for d in range(DEEP):
                    for ref in (u_0, u_a, u_b, k_row):
                        ref[top + d, at, :] = zero_plane
                    w_row[top + d, at, :] = zero_plane + half
                return c

            lax.fori_loop(0, length // SUB, clear, 0)

    def relay_heat(row, g, at):
        u_0[DEEP + row, own, :] = u_nat[g, at, :].T

    def relay_rest(row, g, at):
        k = k_nat[g, at, :]
        marked = jnp.where(s_nat[g, at, :] != 0, -k, k).T
        k_row[DEEP + row, own, :] = jnp.abs(marked)
        w_row[DEEP + row, own, :] = jnp.where(marked < 0.0, zero, half)

    def place(row):
        return row, row // SUB, pl.ds(row % SUB, LANES, stride=SUB)

    def relay_k(row, g, at):
        k_row[DEEP + row, own, :] = k_nat[g, at, :].T

    def relay_mark(row, g, at):
        w_row[DEEP + row, own, :] = jnp.where(s_nat[g, at, :] != 0, zero, half).T

    def pair(r):
        return place(r), place(rows - 1 - r)

    def relay_range(relay, lo):
        amount = rows - 2 * lo
        step = max(d for d in range(1, 16) if amount % d == 0)

        def body(i, c):
            for q in range(step):
                relay(*place(lo + i * step + q))
            return c

        lax.fori_loop(0, amount // step, body, 0)

    def first_copy(m, which, side, arriving):
        lo, hi = CHUNKS[m]
        if which == 0:
            ref, lo, hi = u_0, 0, ROUNDS[0]
        elif which == 1:
            ref = k_row
        else:
            ref, lo, hi = w_row, max(lo - 1, 0), hi - 1
        if hi <= lo:
            return None
        mine = span_at(side, lo, hi)
        theirs = pick(side, DEEP + rows + lo, DEEP - hi)
        halo = pick(side, DEEP - hi, DEEP + rows + lo)
        src = ref.at[pl.ds(halo if arriving else mine, hi - lo), own]
        dst = ref.at[pl.ds(halo if arriving else theirs, hi - lo), own]
        other = side if arriving else 1 - side
        return pltpu.make_async_remote_copy(
            src_ref=src, dst_ref=dst,
            send_sem=first_sems.at[n, side], recv_sem=first_sems.at[m, other],
            device_id=(seg, tile + pick(side, -1, 1)), device_id_type=MESH,
        )

    def first_fields(m):
        return [w for w in range(3) if (w or m == 0) and (w == 0 or CHUNKS[m][1] > CHUNKS[m][0])]

    def rows_in(m, which):
        lo, hi = CHUNKS[m]
        if which == 0:
            return ROUNDS[0] if m == 0 else 0
        return hi - lo if which == 1 else max(hi - 1, 0) - max(lo - 1, 0)

    def first_send(m, side):
        @pl.when(there_is(side))
        def _():
            for which in first_fields(m):
                copy = first_copy(m, which, side, False)
                if copy is not None:
                    copy.start()

    def col_copy(side, part):
        at = (pl.ds(0, 1), pl.ds(groups - 1, 1), pl.ds(1, groups - 2))[part]
        return pltpu.make_async_remote_copy(
            src_ref=col_out.at[side, :, at], dst_ref=col_in.at[1 - side, :, at],
            send_sem=col_sems.at[0, side], recv_sem=col_sems.at[1 + part // 2, 1 - side],
            device_id=(seg + side_step[side], tile), device_id_type=MESH,
        )

    def corner_copy(side, vert):
        g = 0 if vert == 0 else groups - 1
        return pltpu.make_async_remote_copy(
            src_ref=col_out.at[side, :, g], dst_ref=corner_in.at[1 - side, 1 - vert],
            send_sem=corner_sems.at[0, side, vert], recv_sem=corner_sems.at[1, 1 - side, 1 - vert],
            device_id=(seg + side_step[side], tile + side_step[vert]), device_id_type=MESH,
        )

    for g in ends:
        load(2, g).start()
    for which in range(3):
        load(which, 1, groups - 2).start()

    loaded(col_out.at[:, pl.ds(0, 2)], edge_sem.at[0])
    loaded(marks_in, edge_sem.at[1])
    for side in range(2):
        for g in range(groups):
            col_out[side, 2, g] = jnp.where(marks_in[side, g] != 0, zero, half)
    pl.semaphore_wait(barrier, count)
    for side in range(2):
        for vert in range(2):
            @pl.when(has_side[side])
            def _(side=side, vert=vert):
                col_copy(side, vert).start()

            @pl.when(both(has_side[side], has_row[vert]))
            def _(side=side, vert=vert):
                corner_copy(side, vert).start()

    for side in range(2):
        @pl.when(has_side[side])
        def _(side=side):
            col_copy(side, 2).start()

    loaded(u_nat.at[pl.ds(0, 4)], load_sem.at[0])
    for where in pair(0):
        relay_heat(*where)
        relay_k(*where)
    for side in range(2):
        first_send(0, side)
    loaded(s_nat.at[pl.ds(0, 2)], load_sem.at[1])
    for where in pair(0):
        relay_mark(*where)
    for r in range(1, soon):
        for where in pair(r):
            relay_rest(*where)
    for side in range(2):
        first_send(1, side)
    for r in range(1, soon + 1):
        for where in pair(r):
            relay_heat(*where)
    for where in pair(soon):
        relay_rest(*where)
    for which in range(3):
        load(which, 1, groups - 2).wait()
    relay_range(relay_heat, soon + 1)
    relay_range(relay_rest, soon + 1)

    def prepare(start, amount, halo=None, first=0, end=parts + 2, unroll=1, inner=False):
        def body(g, c):
            base = pl.multiple_of(g * SUB, SUB) + PAD
            at = pl.ds(base, SUB)
            if not inner:
                cell = base - own_at + sublane
                outside = both(both(seg == 0, first_lane), cell < 0)
                outside = jnp.logical_or(outside, both(both(seg == n_seg - 1, last_lane), cell >= LANES))
                inside = jnp.logical_not(outside)
            here = k_row[start, at, :]
            north = here + k_row[start - 1, at, :]
            for i in range(amount):
                row = start + i
                below = k_row[row + 1, at, :]
                weight = w_row[row, at, :]
                if not inner:
                    live = inside
                    if halo is not None:
                        live = both(live, halo(i))
                    weight = jnp.where(live, weight, zero)
                south = here + below
                cw = weight * (here + k_row[row, pl.ds(base - 1, SUB), :])
                ce = weight * (here + k_row[row, pl.ds(base + 1, SUB), :])
                for t, term in enumerate((ce, cw, weight * north, weight * south)):
                    coef[row, pl.ds(pl.multiple_of(g * TERM_ROWS, SUB) + t * SUB, SUB), :] = term
                here, north = below, south
            return c

        lax.fori_loop(first, end, body, 0, unroll=unroll)

    def field(level):
        return u_0 if level == 0 else (u_a if level % 2 == 1 else u_b)

    def advance(j, ranges, unroll=1, first=None, end=None):
        src, dst = field(j - 1), field(j)
        last = j == STEPS

        def body(g, c):
            base = pl.multiple_of(g * SUB, SUB) + PAD
            at = pl.ds(base, SUB)
            for start, amount in ranges:
                here = src[start, at, :]
                rise = here - src[start - 1, at, :]
                for i in range(amount):
                    row = start + i
                    below = src[row + 1, at, :]
                    ce, cw, cn, cs = (
                        coef[row, pl.ds(pl.multiple_of(g * TERM_ROWS, SUB) + t * SUB, SUB), :] for t in range(TERMS)
                    )
                    fall = below - here
                    new = here + (
                        (cs * fall - cn * rise)
                        + (ce * (src[row, pl.ds(base + 1, SUB), :] - here) + cw * (src[row, pl.ds(base - 1, SUB), :] - here))
                    )
                    if j == 1:
                        new = jnp.where(w_row[row, at, :] == 0.0, jnp.float32(1.0), new)
                    dst[row, at, :] = new
                    here, rise = below, fall
            return c

        first = (1 if last else 0) if first is None else first
        end = parts + (1 if last else 2) if end is None else end
        lax.fori_loop(first, end, body, 0, unroll=unroll)

    prepare(DEEP + 1, rows - 2, first=2, end=parts, inner=True)
    advance(1, [(DEEP + 1, rows - 2)], first=2, end=parts)

    row_refs = (u_0, k_row, w_row)

    absent = jnp.where((lane // SUB) % FIELDS == FIELDS - 1, half, zero)
    absent_col = jnp.where(lane >= (FIELDS - 1) * rows, half, zero)

    def packed_of(ref, side, found=None):
        a, b = ref.shape[1:3]
        tiles_of = [
            zero_plane if found is not None and q not in found else ref[side, p, q] for p in range(a) for q in range(b)
        ]
        turned = jnp.concatenate(tiles_of + [zero_plane] * (parts - a * b)).T
        return turned[-SUB:] if side == 0 else turned[:SUB]

    def patch(ref, row, side, packed, at_lane):
        end = ref[row, edge_at[1 - side]:edge_at[1 - side] + SUB, :]
        end = pltpu.roll(end, (1, LANES - 1)[side], 1)
        got = pltpu.roll(packed, (edge_id[side] - at_lane) % LANES, 1)
        ref[row, halo_at[side]:halo_at[side] + SUB, :] = jnp.where(edge_lane[side], got, end)

    def col_wait(which, wanted):
        for side in range(2):
            @pl.when(has_side[side])
            def _(side=side):
                part = pl.ds(0, wanted)
                pltpu.make_async_remote_copy(
                    src_ref=col_in.at[side, :, part], dst_ref=col_in.at[side, :, part],
                    send_sem=col_sems.at[0, side], recv_sem=col_sems.at[which, side],
                    device_id=(seg + side_step[side], tile), device_id_type=MESH,
                ).wait_recv()

    col_wait(1, 2)
    def patch_rows(which_rows, found):
        packed_col = [jnp.where(has_side[side], packed_of(col_in, side, found), absent_col) for side in range(2)]
        for side in range(2):
            for r in which_rows:
                for which, ref in enumerate(row_refs):
                    patch(ref, DEEP + r, side, packed_col[side], which * rows + r)

    def sides_of(start, amount):
        for first, end in ((0, 2), (parts, parts + 2)):
            prepare(start, amount, first=first, end=end, unroll=2 if amount < SUB else 1)
            advance(1, [(start, amount)], first=first, end=end, unroll=2 if amount < SUB else 1)

    at_ends = list(range(soon + 1))
    patch_rows(at_ends + [rows - 1 - r for r in at_ends], ends)
    for side in range(2):
        sides_of(span_at(side, 1, soon), soon - 1)

    def row_copy(m, side, early, arriving=False):
        cut = min(ROUNDS[m - 1], ROUNDS[m])
        part = pl.ds(cut, ROUNDS[m] - cut) if early else pl.ds(0, cut)
        other = side if arriving else 1 - side
        return pltpu.make_async_remote_copy(
            src_ref=row_out.at[m - 1, side, part], dst_ref=row_in.at[m - 1, other, part],
            send_sem=row_sems.at[0, m - 1, side], recv_sem=row_sems.at[1, m - 1, other],
            device_id=(seg, tile + pick(side, -1, 1)), device_id_type=MESH,
        )

    def row_whole(m, side):
        part = pl.ds(0, ROUNDS[m])
        return pltpu.make_async_remote_copy(
            src_ref=row_out.at[m - 1, side, part], dst_ref=row_in.at[m - 1, side, part],
            send_sem=row_sems.at[0, m - 1, side], recv_sem=row_sems.at[1, m - 1, side],
            device_id=(seg, tile + 2 * side - 1), device_id_type=MESH,
        )

    def is_early(m):
        return ROUNDS[m] > ROUNDS[m - 1]

    def row_send(m, side, early):
        cut = min(ROUNDS[m - 1], ROUNDS[m])
        src = field(START[m])

        @pl.when(there_is(side))
        def _():
            for r in range(cut, ROUNDS[m]) if early else range(cut):
                row_out[m - 1, side, r, :, :] = src[row_at(side, r), wide, :]
            row_copy(m, side, early).start()

    def row_take(m, side):
        dst = field(START[m])

        @pl.when(there_is(side))
        def _():
            row_whole(m, side).wait_recv()
            for r in range(ROUNDS[m]):
                dst[row_at(side, -1 - r), wide, :] = row_in[m - 1, side, r, :, :]

    def halo_rows(m, side):
        lo, hi = CHUNKS[m]

        @pl.when(there_is(side))
        def _():
            total = sum(rows_in(m, which) for which in range(FIELDS))
            landed = k_row.at[pl.ds(0, total), own]
            pltpu.make_async_remote_copy(
                src_ref=landed, dst_ref=landed, send_sem=first_sems.at[n, side], recv_sem=first_sems.at[m, side],
                device_id=(seg, tile + 2 * side - 1), device_id_type=MESH,
            ).wait_recv()
            for side_of in range(2):
                packed = packed_ref[side_of]
                for which, ref in enumerate(row_refs):
                    if which not in first_fields(m):
                        continue
                    a, b = (lo, hi) if which == 1 else (0, ROUNDS[0]) if which == 0 else (max(lo - 1, 0), hi - 1)
                    for r in range(a, b):
                        at_lane = pick(side, SUB - 1 - r, per_group + r) + which * SUB
                        patch(ref, row_at(side, -1 - r), side_of, packed, at_lane)

        low, high = -(hi - 1), (1 if m == 0 else -(lo - 1))
        start, amount = span_at(side, low, high), high - low

        def halo(i):
            is_halo = jnp.logical_or(start + i < DEEP, start + i >= DEEP + rows)
            return jnp.logical_or(jnp.logical_not(is_halo), there_is(side))

        prepare(start, amount, halo, unroll=6)

    done = {1: 1}
    early_sent = {1}

    def note(j, low):
        done[j] = low
        for m in range(1, n):
            if m not in early_sent and is_early(m) and START[m] == j and low <= ROUNDS[m - 1]:
                early_sent.add(m)
                for side in range(2):
                    row_send(m, side, True)

    def step_all(j, low):
        if j not in done:
            advance(j, [(DEEP + low, rows - 2 * low)])
        elif done[j] > low:
            amount = done[j] - low
            advance(j, [(span_at(side, low, done[j]), amount) for side in range(2)], unroll=2)
        note(j, low)

    def give(row):
        out[row // SUB, pl.ds(row % SUB, LANES, stride=SUB), :] = field(STEPS)[DEEP + row, own, :].T

    for side in range(2):
        row_send(1, side, True)

    for side in range(2):
        for vert in range(2):
            @pl.when(both(has_side[side], has_row[vert]))
            def _(side=side, vert=vert):
                corner_copy(1 - side, 1 - vert).wait_recv()
        packed_ref[side] = jnp.where(has_side[side], packed_of(corner_in, side), absent)

    reached, rounds_met = 0, []
    for what, arg in PLAN:
        if what == "fill":
            for j in range(START[reached] + 1, arg + 1):
                step_all(j, j - START[reached])
        elif what == "give":
            edge = ROUNDS[n - 1]

            def give_more(i, c, edge=edge):
                give(edge + i)
                return c

            lax.fori_loop(0, rows - 2 * edge, give_more, 0, unroll=rows - 2 * edge)
        else:
            m, side = arg, near if what == "near" else far
            if m:
                row_take(m, side)
            if CHUNKS[m][1] > CHUNKS[m][0]:
                halo_rows(m, side)
            for j in range(START[m] + 1, START[m + 1] + 1):
                low, high = j - START[m + 1], j - START[m]
                advance(j, [(span_at(side, low, high), high - low)], unroll=6 if j < STEPS else 4)
            if m + 1 < n:
                row_send(m + 1, side, False)
                if m + 2 < n:
                    first_send(m + 2, side)
            else:
                for i in range(ROUNDS[m]):
                    give(span_at(side, 0, ROUNDS[m]) - DEEP + i)
            rounds_met.append(m)
            if rounds_met.count(m) == 2:
                reached = m + 1
                if m == 0:
                    col_wait(2, groups - 2)
                    patch_rows(range(soon + 1, rows - soon - 1), range(groups))
                    sides_of(DEEP + soon, rows - 2 * soon)
                for j in range(START[m] + 1, START[m + 1] + 1):
                    note(j, j - START[m + 1])

    for side in range(2):
        @pl.when(has_side[side])
        def _(side=side):
            pltpu.make_async_remote_copy(
                src_ref=col_out.at[side], dst_ref=col_out.at[side],
                send_sem=col_sems.at[0, side], recv_sem=col_sems.at[1, side],
                device_id=(seg + side_step[side], tile), device_id_type=MESH,
            ).wait_send()

        for vert in range(2):
            @pl.when(both(has_side[side], has_row[vert]))
            def _(side=side, vert=vert):
                corner_copy(side, vert).wait_send()

        @pl.when(has_row[side])
        def _(side=side):
            total = sum(rows_in(m, which) for m in range(n) for which in range(FIELDS))
            gone = k_row.at[pl.ds(0, total), own]
            pltpu.make_async_remote_copy(
                src_ref=gone, dst_ref=gone, send_sem=first_sems.at[n, side], recv_sem=first_sems.at[0, side],
                device_id=(seg, tile + side_step[side]), device_id_type=MESH,
            ).wait_send()
            for m in range(1, n):
                row_whole(m, side).wait_send()


def write_out(src, dst, sems):
    copies = [pltpu.make_async_copy(src.at[g], dst.at[g], sems.at[g]) for g in range(src.shape[0])]
    for copy in copies:
        copy.start()
    for copy in copies:
        copy.wait()


def shards(n_seg, n_tile, warmth, conductivity, sources):
    rows, columns = warmth.shape
    blocks = columns // LANES
    groups = rows // SUB

    def planes(a):
        return a.reshape(groups, SUB, blocks, LANES).transpose(0, 2, 1, 3).reshape(groups, -1, LANES)

    flat = (groups, SUB * blocks, LANES)
    f32 = jnp.float32
    length = LANES + 2 * SUB + 2 * PAD
    plane = (rows + 2 * DEEP, length, LANES)
    assert blocks == LANES
    vmem = pltpu.VMEM
    sem = pltpu.SemaphoreType.DMA
    n = len(ROUNDS)
    later = max(n - 1, 1)
    halo = (later, 2, DEEP, LANES + 2 * SUB, LANES)
    out = pl.pallas_call(
        functools.partial(kernel, (rows, blocks, n_seg, n_tile)),
        out_shape=jax.ShapeDtypeStruct(flat, f32),
        in_specs=[pl.BlockSpec(memory_space=pltpu.HBM)] * 3,
        out_specs=pl.BlockSpec(memory_space=pltpu.VMEM),
        scratch_shapes=[
            vmem(flat, f32), vmem(flat, f32), vmem(flat, sources.dtype),
        ] + [vmem(plane, f32)] * 5 + [
            vmem((rows + 2 * DEEP, (LANES // SUB + 2) * TERM_ROWS, LANES), f32),
            vmem((2, groups, SUB, LANES), sources.dtype), vmem((2, FIELDS, groups, SUB, LANES), f32),
            vmem((2, FIELDS, groups, SUB, LANES), f32), vmem((2, 2, FIELDS, SUB, LANES), f32), vmem((2, SUB, LANES), f32),
            vmem(halo, f32), vmem(halo, f32),
            sem((5,)), sem((2,)), sem((3, 2)), sem((2, 2, 2)), sem((n + 1, 2)), sem((2, later, 2)),
        ],
        compiler_params=pltpu.CompilerParams(
            collective_id=0, has_side_effects=True, vmem_limit_bytes=VMEM_KERNEL
        ),
    )(planes(warmth), planes(conductivity), planes(sources))
    out = pl.pallas_call(
        write_out,
        out_shape=jax.ShapeDtypeStruct(flat, f32),
        in_specs=[pl.BlockSpec(memory_space=pl.ANY)],
        out_specs=pl.BlockSpec(memory_space=pltpu.HBM),
        scratch_shapes=[sem((groups,))],
        compiler_params=pltpu.CompilerParams(vmem_limit_bytes=VMEM_LAST),
    )(out)
    return out.reshape(groups, blocks, SUB, LANES).transpose(0, 2, 1, 3).reshape(rows, columns)


def solution(mesh):
    spec = P("tile", "seg")
    return jax.shard_map(
        functools.partial(shards, mesh.shape["seg"], mesh.shape["tile"]),
        mesh=mesh,
        in_specs=(spec, spec, spec),
        out_specs=spec,
        check_vma=False,
    )
```

```python
import functools

import jax
import jax.numpy as jnp
from jax import lax
from jax.experimental import pallas as pl
from jax.experimental.pallas import tpu as pltpu
from jax.sharding import PartitionSpec as P

STEPS = 8
ROUNDS = (1, 3, 4)
PLAN = (
    ("far", 0), ("near", 0), ("fill", 4), ("near", 1), ("far", 1), ("fill", 8), ("give", 0), ("near", 2), ("far", 2),
)
assert ROUNDS[0] == 1 and ROUNDS[1] > 1
START = tuple(sum(ROUNDS[:m]) for m in range(len(ROUNDS) + 1))
DEEP = max(ROUNDS)
STEP_SIZE = 0.24
LANES = 128
SUB = 8
MESH = pl.DeviceIdType.MESH

PAD = 16
TERMS = 4
VMEM_KERNEL = 50 * 1024 * 1024
VMEM_LAST = 1024 * 1024
TERM_ROWS = 5 * SUB
FIELDS = 3


def chunks():
    have, found = 0, []
    for d in ROUNDS:
        found.append((have, max(have, d)))
        have = max(have, d)
    return found


CHUNKS = chunks()


def kernel(
    sizes, u_hbm, k_hbm, s_hbm, out,
    u_nat, k_nat, s_nat,
    u_0, u_a, u_b, k_row, w_row, coef,
    marks_in, col_out, col_in, corner_in, packed_ref, row_out, row_in,
    load_sem, edge_sem, col_sems, corner_sems, first_sems, row_sems,
):
    rows, blocks, n_seg, n_tile = sizes
    groups = rows // SUB
    n = len(ROUNDS)
    soon = ROUNDS[1]
    seg, tile = lax.axis_index("seg"), lax.axis_index("tile")
    lane = lax.broadcasted_iota(jnp.int32, (SUB, LANES), 1)
    sublane = lax.broadcasted_iota(jnp.int32, (SUB, LANES), 0)
    first_lane, last_lane = lane == 0, lane == LANES - 1
    has_side = (seg > 0, seg < n_seg - 1)
    has_row = (tile > 0, tile < n_tile - 1)
    side_step = (-1, 1)
    own_at = PAD + SUB
    halo_at = (PAD, own_at + LANES)
    edge_at = (own_at, own_at + LANES - SUB)
    edge_lane = (first_lane, last_lane)
    edge_id = (0, LANES - 1)
    parts = LANES // SUB
    length = LANES + 2 * SUB + 2 * PAD
    zero, half = jnp.float32(0.0), jnp.float32(0.5 * STEP_SIZE)
    own = pl.ds(own_at, LANES)
    wide = pl.ds(PAD, LANES + 2 * SUB)
    per_group = FIELDS * SUB
    near = 1 - tile % 2
    far = tile % 2

    def both(a, b):
        return jnp.logical_and(a, b)

    def there_is(side):
        other = tile + 2 * side - 1
        return both(other >= 0, other < n_tile)

    def pick(side, a, b):
        return a + side * (b - a)

    def span_at(side, lo, hi):
        return pick(side, DEEP + lo, DEEP + rows - hi)

    def row_at(side, r):
        return pick(side, DEEP + r, DEEP + rows - 1 - r)

    barrier = pltpu.get_barrier_semaphore()
    count = jnp.int32(0)
    for ds in (-1, 0, 1):
        for dt in (-1, 0, 1):
            if ds == 0 and dt == 0:
                continue
            there = jnp.bool_(True)
            if ds:
                there = has_side[(ds + 1) // 2]
            if dt:
                there = both(there, has_row[(dt + 1) // 2])
            count = count + there.astype(jnp.int32)

            @pl.when(there)
            def _(ds=ds, dt=dt):
                pl.semaphore_signal(barrier, inc=1, device_id=(seg + ds, tile + dt), device_id_type=MESH)

    span = blocks * SUB
    sources = ((u_hbm, u_nat), (k_hbm, k_nat), (s_hbm, s_nat))

    ends = (0, groups - 1)

    def load(which, g, amount=1):
        src, dst = sources[which]
        part = pl.ds(g, amount)
        sem = load_sem.at[2 + which if amount > 1 else which // 2]
        return pltpu.make_async_copy(src.at[part], dst.at[part], sem)

    def loaded(ref, sem):
        pltpu.make_async_copy(ref, ref, sem).wait()

    def edge_load(which, side):
        at = pl.ds(0 if side == 0 else (blocks - 1) * SUB, SUB)
        dst = marks_in.at[side] if which == 2 else col_out.at[side, which]
        return pltpu.make_async_copy(sources[which][0].at[:, at], dst, edge_sem.at[which // 2])

    for side in range(2):
        for which in range(3):
            edge_load(which, side).start()

    for which in range(2):
        for g in ends:
            load(which, g).start()

    zero_plane = jnp.zeros((SUB, LANES), jnp.float32)
    for side in range(2):
        top = 0 if side == 0 else DEEP + rows

        @pl.when(jnp.logical_not(has_row[side]))
        def _(top=top):
            def clear(j, c):
                at = pl.ds(j * SUB, SUB)
                for d in range(DEEP):
                    for ref in (u_0, u_a, u_b, k_row):
                        ref[top + d, at, :] = zero_plane
                    w_row[top + d, at, :] = zero_plane + half
                return c

            lax.fori_loop(0, length // SUB, clear, 0)

    def relay_heat(row, g, at):
        u_0[DEEP + row, own, :] = u_nat[g, at, :].T

    def relay_rest(row, g, at):
        k = k_nat[g, at, :]
        marked = jnp.where(s_nat[g, at, :] != 0, -k, k).T
        k_row[DEEP + row, own, :] = jnp.abs(marked)
        w_row[DEEP + row, own, :] = jnp.where(marked < 0.0, zero, half)

    def sign(lo, amount):
        def body(i, c):
            at = pl.ds(pl.multiple_of(i * SUB * SUB, SUB), SUB * SUB)
            for g in range(lo, lo + amount):
                k = k_nat[g, at, :]
                k_nat[g, at, :] = jnp.where(s_nat[g, at, :] != 0, -k, k)
            return c

        lax.fori_loop(0, blocks // SUB, body, 0, unroll=2)

    def relay_signed(row, g, at):
        marked = k_nat[g, at, :].T
        k_row[DEEP + row, own, :] = jnp.abs(marked)
        w_row[DEEP + row, own, :] = jnp.where(marked < 0.0, zero, half)

    def place(row):
        return row, row // SUB, pl.ds(row % SUB, LANES, stride=SUB)

    def relay_k(row, g, at):
        k_row[DEEP + row, own, :] = k_nat[g, at, :].T

    def relay_mark(row, g, at):
        w_row[DEEP + row, own, :] = jnp.where(s_nat[g, at, :] != 0, zero, half).T

    def pair(r):
        return place(r), place(rows - 1 - r)

    def relay_range(relay, lo):
        amount = rows - 2 * lo
        step = max(d for d in range(1, 16) if amount % d == 0)

        def body(i, c):
            for q in range(step):
                relay(*place(lo + i * step + q))
            return c

        lax.fori_loop(0, amount // step, body, 0)

    def first_copy(m, which, side, arriving):
        lo, hi = CHUNKS[m]
        if which == 0:
            ref, lo, hi = u_0, 0, ROUNDS[0]
        elif which == 1:
            ref = k_row
        else:
            ref, lo, hi = w_row, max(lo - 1, 0), hi - 1
        if hi <= lo:
            return None
        mine = span_at(side, lo, hi)
        theirs = pick(side, DEEP + rows + lo, DEEP - hi)
        halo = pick(side, DEEP - hi, DEEP + rows + lo)
        src = ref.at[pl.ds(halo if arriving else mine, hi - lo), own]
        dst = ref.at[pl.ds(halo if arriving else theirs, hi - lo), own]
        other = side if arriving else 1 - side
        return pltpu.make_async_remote_copy(
            src_ref=src, dst_ref=dst,
            send_sem=first_sems.at[n, side], recv_sem=first_sems.at[m, other],
            device_id=(seg, tile + pick(side, -1, 1)), device_id_type=MESH,
        )

    def first_fields(m):
        return [w for w in range(3) if (w or m == 0) and (w == 0 or CHUNKS[m][1] > CHUNKS[m][0])]

    def rows_in(m, which):
        lo, hi = CHUNKS[m]
        if which == 0:
            return ROUNDS[0] if m == 0 else 0
        return hi - lo if which == 1 else max(hi - 1, 0) - max(lo - 1, 0)

    def first_send(m, side):
        @pl.when(there_is(side))
        def _():
            for which in first_fields(m):
                copy = first_copy(m, which, side, False)
                if copy is not None:
                    copy.start()

    def col_copy(side, part):
        at = (pl.ds(0, 1), pl.ds(groups - 1, 1), pl.ds(1, groups - 2))[part]
        return pltpu.make_async_remote_copy(
            src_ref=col_out.at[side, :, at], dst_ref=col_in.at[1 - side, :, at],
            send_sem=col_sems.at[0, side], recv_sem=col_sems.at[1 + part // 2, 1 - side],
            device_id=(seg + side_step[side], tile), device_id_type=MESH,
        )

    def corner_copy(side, vert):
        g = 0 if vert == 0 else groups - 1
        return pltpu.make_async_remote_copy(
            src_ref=col_out.at[side, :, g], dst_ref=corner_in.at[1 - side, 1 - vert],
            send_sem=corner_sems.at[0, side, vert], recv_sem=corner_sems.at[1, 1 - side, 1 - vert],
            device_id=(seg + side_step[side], tile + side_step[vert]), device_id_type=MESH,
        )

    for g in ends:
        load(2, g).start()
    for which in range(3):
        load(which, 1, groups - 2).start()

    loaded(col_out.at[:, pl.ds(0, 2)], edge_sem.at[0])
    loaded(marks_in, edge_sem.at[1])
    for side in range(2):
        for g in range(groups):
            col_out[side, 2, g] = jnp.where(marks_in[side, g] != 0, zero, half)
    pl.semaphore_wait(barrier, count)
    for side in range(2):
        for vert in range(2):
            @pl.when(has_side[side])
            def _(side=side, vert=vert):
                col_copy(side, vert).start()

            @pl.when(both(has_side[side], has_row[vert]))
            def _(side=side, vert=vert):
                corner_copy(side, vert).start()

    for side in range(2):
        @pl.when(has_side[side])
        def _(side=side):
            col_copy(side, 2).start()

    loaded(u_nat.at[pl.ds(0, 4)], load_sem.at[0])
    for where in pair(0):
        relay_heat(*where)
        relay_k(*where)
    for side in range(2):
        first_send(0, side)
    loaded(s_nat.at[pl.ds(0, 2)], load_sem.at[1])
    for where in pair(0):
        relay_mark(*where)
    for r in range(1, soon):
        for where in pair(r):
            relay_rest(*where)
    for side in range(2):
        first_send(1, side)
    for r in range(1, soon + 1):
        for where in pair(r):
            relay_heat(*where)
    for where in pair(soon):
        relay_rest(*where)
    for g in ends:
        sign(g, 1)
    for which in range(3):
        load(which, 1, groups - 2).wait()
    sign(1, groups - 2)
    relay_range(relay_heat, soon + 1)
    relay_range(relay_signed, soon + 1)

    def prepare(start, amount, halo=None, first=0, end=parts + 2, unroll=1, inner=False):
        def body(g, c):
            base = pl.multiple_of(g * SUB, SUB) + PAD
            at = pl.ds(base, SUB)
            if not inner:
                cell = base - own_at + sublane
                outside = both(both(seg == 0, first_lane), cell < 0)
                outside = jnp.logical_or(outside, both(both(seg == n_seg - 1, last_lane), cell >= LANES))
                inside = jnp.logical_not(outside)
            here = k_row[start, at, :]
            north = here + k_row[start - 1, at, :]
            for i in range(amount):
                row = start + i
                below = k_row[row + 1, at, :]
                weight = w_row[row, at, :]
                if not inner:
                    live = inside
                    if halo is not None:
                        live = both(live, halo(i))
                    weight = jnp.where(live, weight, zero)
                south = here + below
                cw = weight * (here + k_row[row, pl.ds(base - 1, SUB), :])
                ce = weight * (here + k_row[row, pl.ds(base + 1, SUB), :])
                for t, term in enumerate((ce, cw, weight * north, weight * south)):
                    coef[row, pl.ds(pl.multiple_of(g * TERM_ROWS, SUB) + t * SUB, SUB), :] = term
                here, north = below, south
            return c

        lax.fori_loop(first, end, body, 0, unroll=unroll)

    def field(level):
        return u_0 if level == 0 else (u_a if level % 2 == 1 else u_b)

    def advance(j, ranges, unroll=1, first=None, end=None):
        src, dst = field(j - 1), field(j)
        last = j == STEPS

        def body(g, c):
            base = pl.multiple_of(g * SUB, SUB) + PAD
            at = pl.ds(base, SUB)
            for start, amount in ranges:
                here = src[start, at, :]
                rise = here - src[start - 1, at, :]
                for i in range(amount):
                    row = start + i
                    below = src[row + 1, at, :]
                    ce, cw, cn, cs = (
                        coef[row, pl.ds(pl.multiple_of(g * TERM_ROWS, SUB) + t * SUB, SUB), :] for t in range(TERMS)
                    )
                    fall = below - here
                    new = here + (
                        (cs * fall - cn * rise)
                        + (ce * (src[row, pl.ds(base + 1, SUB), :] - here) + cw * (src[row, pl.ds(base - 1, SUB), :] - here))
                    )
                    if j == 1:
                        new = jnp.where(w_row[row, at, :] == 0.0, jnp.float32(1.0), new)
                    dst[row, at, :] = new
                    here, rise = below, fall
            return c

        first = (1 if last else 0) if first is None else first
        end = parts + (1 if last else 2) if end is None else end
        lax.fori_loop(first, end, body, 0, unroll=unroll)

    prepare(DEEP + 1, rows - 2, first=2, end=parts, inner=True)
    advance(1, [(DEEP + 1, rows - 2)], first=2, end=parts)

    row_refs = (u_0, k_row, w_row)

    absent = jnp.where((lane // SUB) % FIELDS == FIELDS - 1, half, zero)
    absent_col = jnp.where(lane >= (FIELDS - 1) * rows, half, zero)

    def packed_of(ref, side, found=None):
        a, b = ref.shape[1:3]
        tiles_of = [
            zero_plane if found is not None and q not in found else ref[side, p, q] for p in range(a) for q in range(b)
        ]
        turned = jnp.concatenate(tiles_of + [zero_plane] * (parts - a * b)).T
        return turned[-SUB:] if side == 0 else turned[:SUB]

    def patch(ref, row, side, packed, at_lane):
        end = ref[row, edge_at[1 - side]:edge_at[1 - side] + SUB, :]
        end = pltpu.roll(end, (1, LANES - 1)[side], 1)
        got = pltpu.roll(packed, (edge_id[side] - at_lane) % LANES, 1)
        ref[row, halo_at[side]:halo_at[side] + SUB, :] = jnp.where(edge_lane[side], got, end)

    def col_wait(which, wanted):
        for side in range(2):
            @pl.when(has_side[side])
            def _(side=side):
                part = pl.ds(0, wanted)
                pltpu.make_async_remote_copy(
                    src_ref=col_in.at[side, :, part], dst_ref=col_in.at[side, :, part],
                    send_sem=col_sems.at[0, side], recv_sem=col_sems.at[which, side],
                    device_id=(seg + side_step[side], tile), device_id_type=MESH,
                ).wait_recv()

    col_wait(1, 2)
    def patch_rows(which_rows, found):
        packed_col = [jnp.where(has_side[side], packed_of(col_in, side, found), absent_col) for side in range(2)]
        for side in range(2):
            for r in which_rows:
                for which, ref in enumerate(row_refs):
                    patch(ref, DEEP + r, side, packed_col[side], which * rows + r)

    def sides_of(start, amount):
        for first, end in ((0, 2), (parts, parts + 2)):
            prepare(start, amount, first=first, end=end, unroll=2 if amount < SUB else 1)
            advance(1, [(start, amount)], first=first, end=end, unroll=2 if amount < SUB else 1)

    at_ends = list(range(soon + 1))
    patch_rows(at_ends + [rows - 1 - r for r in at_ends], ends)
    for side in range(2):
        sides_of(span_at(side, 1, soon), soon - 1)

    def row_copy(m, side, early, arriving=False):
        cut = min(ROUNDS[m - 1], ROUNDS[m])
        part = pl.ds(cut, ROUNDS[m] - cut) if early else pl.ds(0, cut)
        other = side if arriving else 1 - side
        return pltpu.make_async_remote_copy(
            src_ref=row_out.at[m - 1, side, part], dst_ref=row_in.at[m - 1, other, part],
            send_sem=row_sems.at[0, m - 1, side], recv_sem=row_sems.at[1, m - 1, other],
            device_id=(seg, tile + pick(side, -1, 1)), device_id_type=MESH,
        )

    def row_whole(m, side):
        part = pl.ds(0, ROUNDS[m])
        return pltpu.make_async_remote_copy(
            src_ref=row_out.at[m - 1, side, part], dst_ref=row_in.at[m - 1, side, part],
            send_sem=row_sems.at[0, m - 1, side], recv_sem=row_sems.at[1, m - 1, side],
            device_id=(seg, tile + 2 * side - 1), device_id_type=MESH,
        )

    def is_early(m):
        return ROUNDS[m] > ROUNDS[m - 1]

    def row_send(m, side, early):
        cut = min(ROUNDS[m - 1], ROUNDS[m])
        src = field(START[m])

        @pl.when(there_is(side))
        def _():
            for r in range(cut, ROUNDS[m]) if early else range(cut):
                row_out[m - 1, side, r, :, :] = src[row_at(side, r), wide, :]
            row_copy(m, side, early).start()

    def row_take(m, side):
        dst = field(START[m])

        @pl.when(there_is(side))
        def _():
            row_whole(m, side).wait_recv()
            for r in range(ROUNDS[m]):
                dst[row_at(side, -1 - r), wide, :] = row_in[m - 1, side, r, :, :]

    def halo_rows(m, side):
        lo, hi = CHUNKS[m]

        @pl.when(there_is(side))
        def _():
            total = sum(rows_in(m, which) for which in range(FIELDS))
            landed = k_row.at[pl.ds(0, total), own]
            pltpu.make_async_remote_copy(
                src_ref=landed, dst_ref=landed, send_sem=first_sems.at[n, side], recv_sem=first_sems.at[m, side],
                device_id=(seg, tile + 2 * side - 1), device_id_type=MESH,
            ).wait_recv()
            for side_of in range(2):
                packed = packed_ref[side_of]
                for which, ref in enumerate(row_refs):
                    if which not in first_fields(m):
                        continue
                    a, b = (lo, hi) if which == 1 else (0, ROUNDS[0]) if which == 0 else (max(lo - 1, 0), hi - 1)
                    for r in range(a, b):
                        at_lane = pick(side, SUB - 1 - r, per_group + r) + which * SUB
                        patch(ref, row_at(side, -1 - r), side_of, packed, at_lane)

        low, high = -(hi - 1), (1 if m == 0 else -(lo - 1))
        start, amount = span_at(side, low, high), high - low

        def halo(i):
            is_halo = jnp.logical_or(start + i < DEEP, start + i >= DEEP + rows)
            return jnp.logical_or(jnp.logical_not(is_halo), there_is(side))

        prepare(start, amount, halo, unroll=6)

    done = {1: 1}
    early_sent = {1}

    def note(j, low):
        done[j] = low
        for m in range(1, n):
            if m not in early_sent and is_early(m) and START[m] == j and low <= ROUNDS[m - 1]:
                early_sent.add(m)
                for side in range(2):
                    row_send(m, side, True)

    def step_all(j, low):
        if j not in done:
            advance(j, [(DEEP + low, rows - 2 * low)])
        elif done[j] > low:
            amount = done[j] - low
            advance(j, [(span_at(side, low, done[j]), amount) for side in range(2)], unroll=2)
        note(j, low)

    def give(row):
        out[row // SUB, pl.ds(row % SUB, LANES, stride=SUB), :] = field(STEPS)[DEEP + row, own, :].T

    for side in range(2):
        row_send(1, side, True)

    for side in range(2):
        for vert in range(2):
            @pl.when(both(has_side[side], has_row[vert]))
            def _(side=side, vert=vert):
                corner_copy(1 - side, 1 - vert).wait_recv()
        packed_ref[side] = jnp.where(has_side[side], packed_of(corner_in, side), absent)

    reached, rounds_met = 0, []
    for what, arg in PLAN:
        if what == "fill":
            for j in range(START[reached] + 1, arg + 1):
                step_all(j, j - START[reached])
        elif what == "give":
            edge = ROUNDS[n - 1]

            def give_more(i, c, edge=edge):
                give(edge + i)
                return c

            lax.fori_loop(0, rows - 2 * edge, give_more, 0, unroll=rows - 2 * edge)
        else:
            m, side = arg, near if what == "near" else far
            if m:
                row_take(m, side)
            if CHUNKS[m][1] > CHUNKS[m][0]:
                halo_rows(m, side)
            for j in range(START[m] + 1, START[m + 1] + 1):
                low, high = j - START[m + 1], j - START[m]
                advance(j, [(span_at(side, low, high), high - low)], unroll=6 if j < STEPS else 4)
            if m + 1 < n:
                row_send(m + 1, side, False)
                if m + 2 < n:
                    first_send(m + 2, side)
            else:
                for i in range(ROUNDS[m]):
                    give(span_at(side, 0, ROUNDS[m]) - DEEP + i)
            rounds_met.append(m)
            if rounds_met.count(m) == 2:
                reached = m + 1
                if m == 0:
                    col_wait(2, groups - 2)
                    patch_rows(range(soon + 1, rows - soon - 1), range(groups))
                    sides_of(DEEP + soon, rows - 2 * soon)
                for j in range(START[m] + 1, START[m + 1] + 1):
                    note(j, j - START[m + 1])

    for side in range(2):
        @pl.when(has_side[side])
        def _(side=side):
            pltpu.make_async_remote_copy(
                src_ref=col_out.at[side], dst_ref=col_out.at[side],
                send_sem=col_sems.at[0, side], recv_sem=col_sems.at[1, side],
                device_id=(seg + side_step[side], tile), device_id_type=MESH,
            ).wait_send()

        for vert in range(2):
            @pl.when(both(has_side[side], has_row[vert]))
            def _(side=side, vert=vert):
                corner_copy(side, vert).wait_send()

        @pl.when(has_row[side])
        def _(side=side):
            total = sum(rows_in(m, which) for m in range(n) for which in range(FIELDS))
            gone = k_row.at[pl.ds(0, total), own]
            pltpu.make_async_remote_copy(
                src_ref=gone, dst_ref=gone, send_sem=first_sems.at[n, side], recv_sem=first_sems.at[0, side],
                device_id=(seg, tile + side_step[side]), device_id_type=MESH,
            ).wait_send()
            for m in range(1, n):
                row_whole(m, side).wait_send()


def write_out(src, dst, sems):
    copies = [pltpu.make_async_copy(src.at[g], dst.at[g], sems.at[g]) for g in range(src.shape[0])]
    for copy in copies:
        copy.start()
    for copy in copies:
        copy.wait()


def shards(n_seg, n_tile, warmth, conductivity, sources):
    rows, columns = warmth.shape
    blocks = columns // LANES
    groups = rows // SUB

    def planes(a):
        return a.reshape(groups, SUB, blocks, LANES).transpose(0, 2, 1, 3).reshape(groups, -1, LANES)

    flat = (groups, SUB * blocks, LANES)
    f32 = jnp.float32
    length = LANES + 2 * SUB + 2 * PAD
    plane = (rows + 2 * DEEP, length, LANES)
    assert blocks == LANES
    vmem = pltpu.VMEM
    sem = pltpu.SemaphoreType.DMA
    n = len(ROUNDS)
    later = max(n - 1, 1)
    halo = (later, 2, DEEP, LANES + 2 * SUB, LANES)
    out = pl.pallas_call(
        functools.partial(kernel, (rows, blocks, n_seg, n_tile)),
        out_shape=jax.ShapeDtypeStruct(flat, f32),
        in_specs=[pl.BlockSpec(memory_space=pltpu.HBM)] * 3,
        out_specs=pl.BlockSpec(memory_space=pltpu.VMEM),
        scratch_shapes=[
            vmem(flat, f32), vmem(flat, f32), vmem(flat, sources.dtype),
        ] + [vmem(plane, f32)] * 5 + [
            vmem((rows + 2 * DEEP, (LANES // SUB + 2) * TERM_ROWS, LANES), f32),
            vmem((2, groups, SUB, LANES), sources.dtype), vmem((2, FIELDS, groups, SUB, LANES), f32),
            vmem((2, FIELDS, groups, SUB, LANES), f32), vmem((2, 2, FIELDS, SUB, LANES), f32), vmem((2, SUB, LANES), f32),
            vmem(halo, f32), vmem(halo, f32),
            sem((5,)), sem((2,)), sem((3, 2)), sem((2, 2, 2)), sem((n + 1, 2)), sem((2, later, 2)),
        ],
        compiler_params=pltpu.CompilerParams(
            collective_id=0, has_side_effects=True, vmem_limit_bytes=VMEM_KERNEL
        ),
    )(planes(warmth), planes(conductivity), planes(sources))
    out = pl.pallas_call(
        write_out,
        out_shape=jax.ShapeDtypeStruct(flat, f32),
        in_specs=[pl.BlockSpec(memory_space=pl.ANY)],
        out_specs=pl.BlockSpec(memory_space=pltpu.HBM),
        scratch_shapes=[sem((groups,))],
        compiler_params=pltpu.CompilerParams(vmem_limit_bytes=VMEM_LAST),
    )(out)
    return out.reshape(groups, blocks, SUB, LANES).transpose(0, 2, 1, 3).reshape(rows, columns)


def solution(mesh):
    spec = P("tile", "seg")
    return jax.shard_map(
        functools.partial(shards, mesh.shape["seg"], mesh.shape["tile"]),
        mesh=mesh,
        in_specs=(spec, spec, spec),
        out_specs=spec,
        check_vma=False,
    )
```
